32 devices in a mesh: row: 8 (over y, x, core), col: 4 (over z).
Axes of the slice: x: 2, y: 2, z: 4, core: 2. Of those that a mesh axis runs over, the one named last changes fastest.
Arguments:
- features: bfloat16 [65536, 256], P(('row', 'col')), may hold values from -6 to 6
- tiles: bfloat16 [8, 4, 768, 128, 128], P('row', 'col'), as said below
- tile_rows: int32 [8, 4, 768], P('row', 'col'), may hold values from 0 to 63
- tile_cols: int32 [8, 4, 768], P('row', 'col'), may hold values from 0 to 127
- valid: int32 [8, 4, 768], P('row', 'col'), may hold values from 0 to 1, as said below
- weight: bfloat16 [256, 256], replicated, may hold values from -0.375 to 0.375
- bias: float32 [256], replicated, may hold values from -3 to 3
Outputs:
- hidden: bfloat16 [65536, 256], P(('row', 'col'))
The draws below stay inside these ranges and needn't reach their ends.
Inputs may be any that keep to these rules, and one draw needn't show every extreme that they name: Each cell holds between 96 and 384 valid slots at any positions; in every draw some cell has exactly 384 valid slots. `tiles`: tile entries are non-negative.
All inputs are finite; a program needn't handle non-finite values.
Results may differ from the reference program's by a relative error of at most 0.0039.
Values may be sent and summed in bfloat16 or wider, within the bound.
A program may use at most 256 MiB of HBM per device.

```python
import jax
import jax.numpy as jnp
from jax import lax

F = 256
TILE = 128
SUB = 2048
TPD = 768
NODES = 65536
N_ROW = 8
N_COL = 4


def draw_tiles(key, part):
    shape = (N_ROW, N_COL, TPD, TILE, TILE)
    spread = (SUB / (TPD * TILE * TILE)) ** 0.5
    values = jnp.minimum(jnp.abs(jax.random.normal(key, shape, jnp.float32)) * spread, 5.0 * spread)
    return values.astype(jnp.bfloat16)


def draw_valid(key, part):
    subkeys = jax.random.split(key, 3)
    cells = N_ROW * N_COL
    shifts = jax.random.randint(subkeys[0], (cells,), 1, 4)
    counts = jnp.right_shift(jnp.full((cells,), TPD, jnp.int32), shifts)
    chosen = jax.random.randint(subkeys[1], (), 0, cells)
    counts = jnp.where(jnp.arange(cells) == chosen, TPD // 2, counts)
    orders = jax.vmap(lambda sub_key: jax.random.permutation(sub_key, TPD))(jax.random.split(subkeys[2], cells))
    valid_flags = (orders < counts[:, None]).astype(jnp.int32)
    return valid_flags.reshape(N_ROW, N_COL, TPD)


def touch_ends(values, own_key, smallest, high):
    shape = values.shape
    index_at = [jax.random.randint(jax.random.fold_in(own_key, axis), (), 0, shape[axis]) for axis in range(len(shape))]
    values = values.at[tuple(index_at)].set(smallest)
    longest = shape.index(max(shape))
    index_at[longest] = (index_at[longest] + 1) % shape[longest]
    return values.at[tuple(index_at)].set(high)


def block_scale(rng, dims, cuts, least, high):
    factor_of, own = 1.0, jax.random.fold_in(rng, 6)
    for dim, shards_of in cuts:
        heights = jnp.exp(jax.random.uniform(jax.random.fold_in(own, dim), (shards_of,), jnp.float32, least / len(cuts), high / len(cuts)))
        factor_of = factor_of * jnp.repeat(heights, dims[dim] // shards_of).reshape([-1 if axis == dim else 1 for axis in range(len(dims))])
    return factor_of


def gaussian(key, extent, scale, limit, pieces=(), kind=jnp.bfloat16):
    entries = jax.random.normal(key, extent, jnp.float32) * scale
    if len(pieces) > 0:
        entries = block_scale(key, extent, pieces, -0.22, 0.18) * entries
    return jnp.clip(entries, min=-limit, max=limit).astype(kind)


def setup_inputs(seed: int = 0) -> dict:
    key_list = jax.random.split(jax.random.key(seed), 8)
    features = gaussian(key_list[0], (NODES, F), 1.0, 6.0, ((0, 32),))
    tiles = draw_tiles(jax.random.fold_in(key_list[7], 71), 0)
    tile_rows = touch_ends(jax.random.randint(key_list[2], (N_ROW, N_COL, TPD), 0, SUB * N_COL // TILE), jax.random.fold_in(key_list[2], 1), 0, (SUB * N_COL // TILE) - 1).astype(jnp.int32)
    tile_cols = touch_ends(jax.random.randint(key_list[3], (N_ROW, N_COL, TPD), 0, SUB * N_ROW // TILE), jax.random.fold_in(key_list[3], 1), 0, (SUB * N_ROW // TILE) - 1).astype(jnp.int32)
    valid = draw_valid(jax.random.fold_in(key_list[7], 71), 0)
    weight = gaussian(key_list[5], (F, F), F ** -0.5, 0.375)
    bias = gaussian(key_list[6], (F,), 0.5, 3.0, (), jnp.float32)
    return {"features": features, "tiles": tiles, "tile_rows": tile_rows, "tile_cols": tile_cols, "valid": valid, "weight": weight, "bias": bias}


def reference(features, tiles, tile_rows, tile_cols, valid, weight, bias):
    row_tiles = SUB * N_COL // TILE
    grouped = features.reshape(N_ROW, N_COL, SUB, F)
    flat_tiles = tiles.reshape(N_ROW * N_COL, TPD, TILE, TILE)
    flat_rows = tile_rows.reshape(N_ROW * N_COL, TPD)
    flat_cols = tile_cols.reshape(N_ROW * N_COL, TPD)
    flat_valid = valid.reshape(N_ROW * N_COL, TPD)

    def one_cell(device):
        column = device % N_COL
        panel = jnp.take(grouped, column, axis=1).reshape(-1, TILE, F)
        chosen = panel[flat_cols[device]]
        products = jnp.einsum("bij,bjf->bif", flat_tiles[device].astype(jnp.float32), chosen.astype(jnp.float32))
        products = products * flat_valid[device].astype(jnp.float32)[:, None, None]
        partial_sum = jnp.zeros((row_tiles, TILE, F), jnp.float32)
        return partial_sum.at[flat_rows[device]].add(products)

    partials = lax.map(one_cell, jnp.arange(N_ROW * N_COL, dtype=jnp.int32))
    totals = jnp.sum(partials.reshape(N_ROW, N_COL, row_tiles, TILE, F), axis=1)
    aggregated = totals.reshape(N_ROW * N_COL * SUB, F).astype(jnp.bfloat16)
    mixed = jnp.dot(aggregated, weight, preferred_element_type=jnp.float32) + bias
    return jnp.maximum(mixed, 0.0).astype(jnp.bfloat16)
```

```python
import functools

import jax
import jax.numpy as jnp
from jax import lax
from jax.experimental import pallas as pl
from jax.experimental.pallas import tpu as pltpu
from jax.sharding import PartitionSpec as P

SLOTS = 32
UNROLL = 8


def spmm_kernel(valid, rows, cols, panel_hbm, tiles_hbm, out_ref,
                slot_list, row_list, col_list, panel, total, ring, ring_sem, panel_sem):
    slot_count = valid.shape[0]
    row_tiles = out_ref.shape[0]
    panel_copy = pltpu.make_async_copy(panel_hbm, panel, panel_sem)
    panel_copy.start()

    def scan(step, count):
        for k in range(UNROLL):
            slot = step * UNROLL + k
            slot_list[count] = slot
            row_list[count] = rows[slot]
            col_list[count] = cols[slot]
            count = count + valid[slot]
        return count

    count = lax.fori_loop(0, slot_count // UNROLL, scan, jnp.int32(0))
    for k in range(UNROLL):
        slot_list[count + k] = 0
        row_list[count + k] = row_tiles
        col_list[count + k] = 0
    steps = (count + UNROLL - 1) // UNROLL
    filled = steps * UNROLL

    def fetch(index):
        place = lax.rem(index, SLOTS)
        return pltpu.make_async_copy(
            tiles_hbm.at[slot_list[index]], ring.at[place], ring_sem.at[place])

    def prime(index, carry):
        @pl.when(index < filled)
        def _():
            fetch(index).start()
        return carry

    lax.fori_loop(0, SLOTS, prime, 0)
    total[...] = jnp.zeros_like(total)
    panel_copy.wait()

    def step_body(step, carry):
        base = step * UNROLL
        for k in range(UNROLL):
            fetch(base + k).wait()
        for k in range(UNROLL):
            index = base + k
            product = jnp.dot(ring[lax.rem(index, SLOTS)], panel[col_list[index]],
                              preferred_element_type=jnp.float32)
            row = row_list[index]
            total[row] = total[row] + product
        for k in range(UNROLL):
            later = base + SLOTS + k

            @pl.when(later < filled)
            def _():
                fetch(later).start()
        return carry

    lax.fori_loop(0, steps, step_body, 0)

    def put(row, carry):
        out_ref[row] = total[row].astype(out_ref.dtype)
        return carry

    lax.fori_loop(0, row_tiles, put, 0)


def spmm(valid, rows, cols, panel, tiles, row_tiles):
    slot_count, tile_size = tiles.shape[0], tiles.shape[1]
    width = panel.shape[2]
    smem = pl.BlockSpec(memory_space=pltpu.SMEM)
    hbm = pl.BlockSpec(memory_space=pl.ANY)
    return pl.pallas_call(
        spmm_kernel,
        out_shape=jax.ShapeDtypeStruct((row_tiles, tile_size, width), jnp.bfloat16),
        in_specs=[smem, smem, smem, hbm, hbm],
        out_specs=pl.BlockSpec(memory_space=pltpu.VMEM),
        scratch_shapes=[
            pltpu.SMEM((slot_count + UNROLL,), jnp.int32),
            pltpu.SMEM((slot_count + UNROLL,), jnp.int32),
            pltpu.SMEM((slot_count + UNROLL,), jnp.int32),
            pltpu.VMEM(panel.shape, jnp.bfloat16),
            pltpu.VMEM((row_tiles + 1, tile_size, width), jnp.float32),
            pltpu.VMEM((SLOTS, tile_size, tile_size), jnp.bfloat16),
            pltpu.SemaphoreType.DMA((SLOTS,)),
            pltpu.SemaphoreType.DMA,
        ],
        compiler_params=pltpu.CompilerParams(vmem_limit_bytes=60 * 2**20),
        cost_estimate=pl.CostEstimate(
            flops=slot_count * tile_size * tile_size * width, bytes_accessed=32 * 2**20,
            transcendentals=0),
    )(valid, rows, cols, panel, tiles)


def on_device(features, tiles, tile_rows, tile_cols, valid, weight, bias):
    sub_rows, width = features.shape
    tile_size = tiles.shape[3]
    row_tiles = sub_rows * lax.axis_size("col") // tile_size
    panel = lax.all_gather(features, "row", axis=0, tiled=True).reshape(-1, tile_size, width)
    partial = spmm(valid[0, 0], tile_rows[0, 0], tile_cols[0, 0], panel, tiles[0, 0], row_tiles)
    summed = lax.psum_scatter(
        partial.reshape(row_tiles * tile_size, width), "col", scatter_dimension=0, tiled=True)
    mixed = jnp.dot(summed, weight, preferred_element_type=jnp.float32) + bias
    return jnp.maximum(mixed, 0.0).astype(jnp.bfloat16)


def solution(mesh):
    return jax.shard_map(
        on_device,
        mesh=mesh,
        in_specs=(
            P(("row", "col"), None),
            P("row", "col", None, None, None),
            P("row", "col", None),
            P("row", "col", None),
            P("row", "col", None),
            P(),
            P(),
        ),
        out_specs=P(("row", "col"), None),
        check_vma=False,
    )
```

```python
import functools

import jax
import jax.numpy as jnp
from jax import lax
from jax.experimental import pallas as pl
from jax.experimental.pallas import tpu as pltpu
from jax.sharding import PartitionSpec as P

SLOTS = 32
UNROLL = 8


def spmm_kernel(valid, rows, cols, panel_hbm, tiles_hbm, total,
                slot_list, row_list, col_list, panel, ring, ring_sem, panel_sem):
    slot_count = valid.shape[2]
    row_tiles = total.shape[0] - 1
    panel_copy = pltpu.make_async_copy(panel_hbm, panel, panel_sem)
    panel_copy.start()

    def scan(step, count):
        for k in range(UNROLL):
            slot = step * UNROLL + k
            slot_list[count] = slot
            row_list[count] = rows[0, 0, slot]
            col_list[count] = cols[0, 0, slot]
            count = count + valid[0, 0, slot]
        return count

    count = lax.fori_loop(0, slot_count // UNROLL, scan, jnp.int32(0))
    for k in range(UNROLL):
        slot_list[count + k] = 0
        row_list[count + k] = row_tiles
        col_list[count + k] = 0
    steps = (count + UNROLL - 1) // UNROLL
    filled = steps * UNROLL

    def fetch(index):
        place = lax.rem(index, SLOTS)
        return pltpu.make_async_copy(
            tiles_hbm.at[0, 0, slot_list[index]], ring.at[place], ring_sem.at[place])

    def prime(index, carry):
        @pl.when(index < filled)
        def _():
            fetch(index).start()
        return carry

    lax.fori_loop(0, SLOTS, prime, 0)
    total[...] = jnp.zeros_like(total)
    panel_copy.wait()

    def step_body(step, carry):
        base = step * UNROLL
        for k in range(UNROLL):
            fetch(base + k).wait()
        for k in range(UNROLL):
            index = base + k
            product = jnp.dot(ring[lax.rem(index, SLOTS)], panel[col_list[index]],
                              preferred_element_type=jnp.float32)
            row = row_list[index]
            total[row] = total[row] + product
        for k in range(UNROLL):
            later = base + SLOTS + k

            @pl.when(later < filled)
            def _():
                fetch(later).start()
        return carry

    lax.fori_loop(0, steps, step_body, 0)


def spmm(valid, rows, cols, panel, tiles, row_tiles):
    slot_count, tile_size = tiles.shape[2], tiles.shape[3]
    width = panel.shape[2]
    smem = pl.BlockSpec(memory_space=pltpu.SMEM)
    hbm = pl.BlockSpec(memory_space=pl.ANY)
    return pl.pallas_call(
        spmm_kernel,
        out_shape=jax.ShapeDtypeStruct((row_tiles + 1, tile_size, width), jnp.float32),
        in_specs=[smem, smem, smem, hbm, hbm],
        out_specs=pl.BlockSpec(memory_space=pltpu.VMEM),
        scratch_shapes=[
            pltpu.SMEM((slot_count + UNROLL,), jnp.int32),
            pltpu.SMEM((slot_count + UNROLL,), jnp.int32),
            pltpu.SMEM((slot_count + UNROLL,), jnp.int32),
            pltpu.VMEM(panel.shape, jnp.bfloat16),
            pltpu.VMEM((SLOTS, tile_size, tile_size), jnp.bfloat16),
            pltpu.SemaphoreType.DMA((SLOTS,)),
            pltpu.SemaphoreType.DMA,
        ],
        compiler_params=pltpu.CompilerParams(vmem_limit_bytes=60 * 2**20),
        cost_estimate=pl.CostEstimate(
            flops=slot_count * tile_size * tile_size * width, bytes_accessed=32 * 2**20,
            transcendentals=0),
    )(valid, rows, cols, panel, tiles)


MESH = pl.DeviceIdType.MESH
PIECES = 2


def gather_steps(features, lane, panel, send_sem, recv_sem, local_sem, rows):
    sub_rows, width = panel.shape[1], panel.shape[2]
    cut = sub_rows // 2
    me = lax.axis_index("row")
    chips = rows // 2
    core, chip = lax.rem(me, 2), me // 2
    partner = chip * 2 + (1 - core)
    own = features.at[:, pl.ds(lane * width, width)]

    def half(ref, k):
        return ref.at[pl.ds(k * cut, cut)]

    def copy(src, block, k, number, target):
        return pltpu.make_async_remote_copy(
            src_ref=src, dst_ref=half(panel.at[block], k), send_sem=send_sem.at[number],
            recv_sem=recv_sem.at[number], device_id={"row": target}, device_id_type=MESH)

    def held(block, k):
        return half(panel.at[block], k)

    if chips == 4:
        over_x, over_y = lax.rem(chip, 2), chip // 2
        x_side = (over_y * 2 + (1 - over_x)) * 2 + core
        y_side = ((1 - over_y) * 2 + over_x) * 2 + core
        across = ((1 - over_y) * 2 + (1 - over_x)) * 2 + core
        peers = [x_side, y_side]
        sources = [x_side, y_side, y_side, x_side]
        own_copies = [copy(half(own, 0), me, 0, 0, x_side), copy(half(own, 1), me, 1, 1, y_side),
                      copy(half(own, 1), me, 1, 2, x_side), copy(half(own, 0), me, 0, 3, y_side)]
        passed = {0: copy(held(x_side, 0), x_side, 0, 4, y_side),
                  1: copy(held(y_side, 1), y_side, 1, 5, x_side)}
        arriving = [(x_side, 0), (y_side, 1), (x_side, 1), (y_side, 0), (across, 0), (across, 1)]
    else:
        peers = [lax.rem(chip + k, chips) * 2 + core for k in range(1, chips)]
        from_peers = [lax.rem(chip + chips - k, chips) * 2 + core for k in range(1, chips)]
        own_copies, passed, arriving = [], {}, []
        for place, (peer, giver) in enumerate(zip(peers, from_peers)):
            for k in range(2):
                own_copies.append(copy(half(own, k), me, k, 2 * place + k, peer))
                arriving.append((giver, k))
    direct = len(arriving)
    started = list(own_copies)
    keep = pltpu.make_async_copy(own, panel.at[me], local_sem)

    def begin():
        for item in own_copies:
            item.start()
        for k in range(2):
            item = copy(half(own, k), me, k, direct + k, partner)
            item.start()
            started.append(item)
        keep.start()

    def receive(number):
        block, k = arriving[number]
        copy(held(block, k), block, k, number, partner).wait_recv()
        if number in passed:
            passed[number].start()
            started.append(passed[number])
        item = copy(held(block, k), block, k, direct + 2 + number, partner)
        item.start()
        started.append(item)

    def finish():
        for number in range(direct + 2):
            copy(held(me, 0), me, 0, direct + number, partner).wait_recv()
        for item in started:
            item.wait_send()
        keep.wait()

    steps = [functools.partial(receive, number) for number in range(direct)]
    return peers + [partner], begin, steps, finish


def reduce_steps(partial, summed, to_right, to_left, from_left, from_right, total, sems, columns):
    tiles_each = summed.shape[0]
    cut = tiles_each // PIECES
    me = lax.axis_index("col")
    right_send, right_recv, left_send, left_recv = sems

    def move(rightward, dest, piece):
        place = dest - 1 if rightward else dest
        outbox, inbox = (to_right, from_left) if rightward else (to_left, from_right)
        send, recv = (right_send, right_recv) if rightward else (left_send, left_recv)
        part = pl.ds(piece * cut, cut)
        inner = (me < dest) if rightward else (me > dest)
        first = (me == 0) if rightward else (me == columns - 1)
        number = place * PIECES + piece
        target = me + 1 if rightward else me - 1
        item = pltpu.make_async_remote_copy(
            src_ref=outbox.at[place, part], dst_ref=inbox.at[place, part],
            send_sem=send.at[number], recv_sem=recv.at[number],
            device_id={"col": target}, device_id_type=MESH)
        here = pl.ds(dest * tiles_each + piece * cut, cut)

        def open_chain():
            @pl.when(first)
            def _():
                outbox[place, part] = partial[here].astype(outbox.dtype)
                item.start()

        def pass_on():
            @pl.when(jnp.logical_and(inner, jnp.logical_not(first)))
            def _():
                item.wait_recv()
                outbox[place, part] = (
                    partial[here] + inbox[place, part].astype(jnp.float32)).astype(outbox.dtype)
                item.start()

        def close_chain():
            @pl.when(me == dest)
            def _():
                item.wait_recv()
                total[part] = total[part] + inbox[place, part].astype(jnp.float32)

        def drain():
            @pl.when(inner)
            def _():
                item.wait_send()

        return open_chain, pass_on, close_chain, drain

    links = []
    for turn in range(columns - 1):
        for piece in range(PIECES):
            links.append(move(True, columns - 1 - turn, piece))
            links.append(move(False, turn, piece))

    def begin():
        for link in links:
            link[0]()
        total[...] = partial[pl.ds(me * tiles_each, tiles_each)]

    def finish():
        for link in links:
            link[2]()
        summed[...] = total[...].astype(summed.dtype)
        for link in links:
            link[3]()

    return begin, [link[1] for link in links], finish


def exchange_kernel(gathering, reducing, lane, rows, columns, *refs):
    refs = list(refs)
    features = refs.pop(0) if gathering else None
    partial = refs.pop(0) if reducing else None
    panel = refs.pop(0) if gathering else None
    summed = refs.pop(0) if reducing else None
    peers, queue = [], []
    if gathering:
        send_sem, recv_sem, local_sem = refs.pop(0), refs.pop(0), refs.pop(0)
        peers, gather_begin, gather_list, gather_finish = gather_steps(
            features, lane, panel, send_sem, recv_sem, local_sem, rows)
    if reducing:
        reduce_begin, reduce_list, reduce_finish = reduce_steps(
            partial, summed, *refs[:5], refs[5:9], columns)

    barrier = pltpu.get_barrier_semaphore()
    for peer in peers:
        pl.semaphore_signal(barrier, inc=1, device_id={"row": peer}, device_id_type=MESH)
    expected = len(peers)
    if reducing:
        me = lax.axis_index("col")

        @pl.when(me > 0)
        def _():
            pl.semaphore_signal(barrier, inc=1, device_id={"col": me - 1}, device_id_type=MESH)

        @pl.when(me < columns - 1)
        def _():
            pl.semaphore_signal(barrier, inc=1, device_id={"col": me + 1}, device_id_type=MESH)

        inside = jnp.logical_and(me > 0, me < columns - 1)

        @pl.when(inside)
        def _():
            pl.semaphore_wait(barrier, expected + 2)

        @pl.when(jnp.logical_not(inside))
        def _():
            pl.semaphore_wait(barrier, expected + 1)
    else:
        pl.semaphore_wait(barrier, expected)

    if gathering:
        gather_begin()
    if reducing:
        reduce_begin()
    gather_queue = list(gather_list) if gathering else []
    reduce_queue = list(reduce_list) if reducing else []
    while gather_queue or reduce_queue:
        for queue in (gather_queue, reduce_queue):
            for _ in range(2):
                if queue:
                    queue.pop(0)()
    if gathering:
        gather_finish()
    if reducing:
        reduce_finish()


def exchange(number, features, lane, partial, width, tile_size, rows, columns):
    gathering, reducing = features is not None, partial is not None
    hbm, vmem = pl.BlockSpec(memory_space=pl.ANY), pl.BlockSpec(memory_space=pltpu.VMEM)
    operands, in_specs, out_shape, out_specs, scratch = [], [], [], [], []
    if gathering:
        sub_rows = features.shape[0]
        operands.append(features)
        in_specs.append(hbm)
        out_shape.append(jax.ShapeDtypeStruct((rows, sub_rows, width), jnp.bfloat16))
        out_specs.append(hbm)
        chips = rows // 2
        copies = 2 * (6 if chips == 4 else 2 * (chips - 1)) + 2
        scratch += [pltpu.SemaphoreType.DMA((copies,)), pltpu.SemaphoreType.DMA((copies,)),
                    pltpu.SemaphoreType.DMA]
    if reducing:
        tiles_each = (partial.shape[0] - 1) // columns
        operands.append(partial)
        in_specs.append(vmem)
        out_shape.append(jax.ShapeDtypeStruct((tiles_each, tile_size, width), jnp.bfloat16))
        out_specs.append(vmem)
        scratch += [pltpu.VMEM((columns - 1, tiles_each, tile_size, width), jnp.bfloat16)] * 4
        scratch += [pltpu.VMEM((tiles_each, tile_size, width), jnp.float32)]
        scratch += [pltpu.SemaphoreType.DMA(((columns - 1) * PIECES,))] * 4
    return pl.pallas_call(
        functools.partial(exchange_kernel, gathering, reducing, lane, rows, columns),
        out_shape=out_shape, in_specs=in_specs, out_specs=out_specs, scratch_shapes=scratch,
        compiler_params=pltpu.CompilerParams(
            collective_id=number, has_side_effects=True, vmem_limit_bytes=60 * 2**20),
    )(*operands)


def on_device(features, tiles, tile_rows, tile_cols, valid, weight, bias):
    sub_rows, channels = features.shape
    tile_size = tiles.shape[3]
    rows, columns = lax.axis_size("row"), lax.axis_size("col")
    row_tiles = sub_rows * columns // tile_size
    width = min(channels, 128)
    lanes = channels // width
    cells = (valid, tile_rows, tile_cols)
    sums, partial = [], None
    for lane in range(lanes + 1):
        results = list(exchange(
            lane, features if lane < lanes else None, lane, partial, width, tile_size, rows, columns))
        if partial is not None:
            sums.append(results.pop().reshape(sub_rows, width))
        if lane < lanes:
            panel = results[0].reshape(-1, tile_size, width)
            partial = spmm(*cells, panel, tiles, row_tiles)
    mixed = bias
    for lane in range(lanes):
        mixed = mixed + jnp.dot(sums[lane], weight[lane * width:(lane + 1) * width],
                                preferred_element_type=jnp.float32)
    return jnp.maximum(mixed, 0.0).astype(jnp.bfloat16)


def solution(mesh):
    return jax.shard_map(
        on_device,
        mesh=mesh,
        in_specs=(
            P(("row", "col"), None),
            P("row", "col", None, None, None),
            P("row", "col", None),
            P("row", "col", None),
            P("row", "col", None),
            P(),
            P(),
        ),
        out_specs=P(("row", "col"), None),
        check_vma=False,
    )
```
